32 devices in a mesh: seq: 8 (over z, core), head: 4 (over y, x).
Axes of the slice: x: 2, y: 2, z: 4, core: 2. Of those that a mesh axis runs over, the one named last changes fastest.
Arguments:
- queries: bfloat16 [1024, 2048], P('seq', 'head'), may hold values from -192 to 192
- keys: bfloat16 [1024, 512], P('seq', 'head'), may hold values from -5 to 5
- values: bfloat16 [1024, 512], P('seq', 'head'), may hold values from -24 to 24
- segments: int32 [1024], replicated, may hold values from 0 to 5, never falling along the last dimension, each value on 1 to 341 neighbouring positions
- out_weight: bfloat16 [2048, 8192], P(None, 'head'), may hold values from -0.125 to 0.125
Outputs:
- mixed: bfloat16 [1024, 8192], P('seq', 'head')
The draws below stay inside these ranges and needn't reach their ends.
All inputs are finite; a program needn't handle non-finite values.
Results may differ from the reference program's by a relative error of at most 0.007.
Values may be sent and summed in bfloat16 or wider, within the bound.
A program may use at most 64 MiB of HBM per device.

```python
import math
import jax
import jax.numpy as jnp
import numpy as np
from jax import lax

D = 8192
HD = 128
GROUP = 4
TOK_DEV = 128
WIN_BLK = 31
KV_HEADS = 4
QH = 16
TOKENS = 1024


def drawn_rows(key):
    key_field = jax.random.normal(jax.random.fold_in(key, 11), (TOKENS, KV_HEADS, HD), jnp.float32)
    key_field = jnp.clip(key_field, -5.0, 5.0)
    return key_field


def draw_keys(key, part):
    key_field = drawn_rows(key)
    return key_field.reshape(TOKENS, KV_HEADS * HD).astype(jnp.bfloat16)


def draw_queries(key, part):
    base = jax.random.normal(jax.random.fold_in(key, 13), (TOKENS, KV_HEADS, GROUP, HD), jnp.float32)
    base = 2.0 * jnp.clip(base, -5.0, 5.0)
    return base.reshape(TOKENS, KV_HEADS * GROUP * HD).astype(jnp.bfloat16)


def level_of(stream_key, shape, shards, least, top_value):
    gain = 1.0
    for dim, shards_of in shards:
        heights = jax.random.uniform(jax.random.fold_in(jax.random.fold_in(stream_key, 6), dim), (shards_of,), jnp.float32, least / len(shards), top_value / len(shards))
        gain = gain * jnp.repeat(jnp.exp(heights), shape[dim] // shards_of).reshape((-1,) + (1,) * (len(shape) - 1 - dim))
    return gain


def split_up(amount, total, bound, slope):
    loads = [(1 << 20) // math.isqrt(grade ** slope) + 1 for grade in range(2, amount + 1)]
    surplus, given = total - bound - (amount - 1), [1] * (amount - 1)
    while surplus > 0:
        movable = [i for i in range(amount - 1) if given[i] < bound]
        mass, left = sum([loads[i] for i in movable]), surplus
        for i in movable:
            more = min(bound - given[i], max(1, left * loads[i] // mass), surplus)
            given[i] = given[i] + more
            surplus = surplus - more
    return np.array([bound] + given)


def ragged_sizes(own_key, count, total, most, lean):
    if count == 2:
        one = jax.random.randint(own_key, (), max(1, total - most), min(most, total - 1) + 1)
        return jnp.stack([one, total - one])
    tallies = jnp.asarray(split_up(count, total, most, lean), jnp.int32)
    pairs = (count - 1) // 2
    donor, receiver = tallies[1:1 + 2 * pairs:2], tallies[2:2 + 2 * pairs:2]
    margin = jnp.minimum(donor - 1, most - receiver)
    passed = jax.random.randint(jax.random.fold_in(own_key, 1), (pairs,), 0, 1 << 20) % (margin + 1)
    tallies = tallies.at[1:1 + 2 * pairs:2].set(donor - passed).at[2:2 + 2 * pairs:2].set(receiver + passed)
    return tallies[jax.random.permutation(jax.random.fold_in(own_key, 2), count)]


def normal_values(own_key, extent, scale, limit, pieces=(), kind=jnp.bfloat16):
    loudness = level_of(own_key, extent, pieces, -0.22, 0.18) if pieces else 1.0
    values = jax.random.normal(own_key, extent, jnp.float32) * scale * loudness
    return jnp.minimum(jnp.maximum(values, -limit), limit).astype(kind)


def setup_inputs(seed: int = 0) -> dict:
    splits = jax.random.split(jax.random.key(seed), 6)
    queries = draw_queries(jax.random.fold_in(splits[5], 71), 0)
    keys = draw_keys(jax.random.fold_in(splits[5], 71), 0)
    values = normal_values(splits[2], (TOKENS, KV_HEADS * HD), 4.0, 24.0, ((0, 8), (1, 4)))
    segments = jnp.searchsorted(jnp.cumsum(ragged_sizes(splits[3], 6, TOKENS, TOKENS // 3, 1)), jnp.arange(TOKENS), side="right").astype(jnp.int32)
    out_weight = normal_values(splits[4], (QH * HD, D), (QH * HD) ** -0.5, 0.125, ((1, 4),))
    return dict(queries=queries, keys=keys, values=values, segments=segments, out_weight=out_weight)


masked_score = -1e+30

def reference(queries, keys, values, segments, out_weight):
    token_total = queries.shape[0]
    kv_heads = keys.shape[1] // HD
    group_size = queries.shape[1] // keys.shape[1]
    window_len = WIN_BLK * TOK_DEV
    length = window_len + TOK_DEV
    padding = jnp.zeros((window_len, keys.shape[1]), keys.dtype)
    keys_padded = jnp.concatenate([padding, keys], axis=0)
    values_padded = jnp.concatenate([padding, values], axis=0)
    seg_whole = segments.astype(jnp.int32)
    seg_padded = jnp.concatenate([jnp.full((window_len,), -1, jnp.int32), seg_whole])
    scaling = 1.0 / math.sqrt(HD)

    def one_block(block_index):
        first_row = (block_index * TOK_DEV).astype(jnp.int32)
        query_block = lax.dynamic_slice_in_dim(queries, first_row, TOK_DEV, 0)
        query_block = query_block.reshape(TOK_DEV, kv_heads, group_size, HD).astype(jnp.float32)
        key_block = lax.dynamic_slice_in_dim(keys_padded, first_row, length, 0)
        key_block = key_block.reshape(length, kv_heads, HD).astype(jnp.float32)
        value_block = lax.dynamic_slice_in_dim(values_padded, first_row, length, 0)
        value_block = value_block.reshape(length, kv_heads, HD).astype(jnp.float32)
        query_pos = first_row + jnp.arange(TOK_DEV, dtype=jnp.int32)
        key_pos = first_row - window_len + jnp.arange(length, dtype=jnp.int32)
        query_seg = lax.dynamic_slice_in_dim(seg_whole, first_row, TOK_DEV, 0)
        key_seg = lax.dynamic_slice_in_dim(seg_padded, first_row, length, 0)
        allowed = key_pos[None, :] <= query_pos[:, None]
        allowed = allowed & (query_pos[:, None] - key_pos[None, :] < window_len)
        allowed = allowed & (key_pos[None, :] >= 0)
        allowed = allowed & (key_seg[None, :] == query_seg[:, None])
        scores = jnp.einsum('tagd,sad->agts', query_block, key_block) * scaling
        scores = jnp.where(allowed[None, None], scores, masked_score)
        row_max = lax.optimization_barrier(jnp.max(scores, axis=-1, keepdims=True))
        weights = jnp.exp(scores - row_max)
        denominator = lax.optimization_barrier(jnp.sum(weights, axis=-1))
        rounded = lax.optimization_barrier(weights.astype(jnp.bfloat16)).astype(jnp.float32)
        numerator = jnp.einsum('agts,sad->tagd', rounded, value_block)
        result = numerator / jnp.transpose(denominator, (2, 0, 1))[..., None]
        return result.reshape(TOK_DEV, kv_heads * group_size * HD).astype(jnp.bfloat16)
    blocks = lax.map(one_block, jnp.arange(token_total // TOK_DEV, dtype=jnp.int32))
    attended = blocks.reshape(token_total, queries.shape[1])
    return jnp.dot(attended, out_weight, preferred_element_type=jnp.float32).astype(jnp.bfloat16)
```

```python
import functools
import math

import jax
import jax.numpy as jnp
from jax import lax
from jax.experimental import pallas as pl
from jax.experimental.pallas import tpu as pltpu
from jax.sharding import PartitionSpec as P

HD = 128
WIN_BLK = 31


masked_score = -1e30


def passed_along(block, axis, distance):
    devices = range(lax.axis_size(axis))
    route = [(i - distance, i) for i in devices if i - distance in devices]
    return lax.ppermute(block, axis, route)


def allowed_keys(segments, query_pos, query_seg, key_first, key_count, window_len):
    key_pos = key_first + jnp.arange(key_count, dtype=jnp.int32)
    clipped = jnp.clip(key_pos, 0, segments.shape[0] - 1)
    key_seg = jnp.take(segments, clipped)
    allowed = key_pos[None, :] <= query_pos[:, None]
    allowed = allowed & (query_pos[:, None] - key_pos[None, :] < window_len)
    allowed = allowed & (key_pos[None, :] >= 0)
    return allowed & (key_seg[None, :] == query_seg[:, None])


def absorb(carry_state, query_heads, key_piece, value_piece, allowed):
    row_max, row_sum, accum = carry_state
    key_count = key_piece.shape[0]
    kv_heads = query_heads.shape[1]
    key_heads = key_piece.reshape(key_count, kv_heads, HD)
    value_heads = value_piece.reshape(key_count, kv_heads, HD)
    scores = jnp.einsum(
        "tagd,sad->agts", query_heads, key_heads, preferred_element_type=jnp.float32
    )
    scores = jnp.where(allowed[None, None], scores * HD ** (-0.5), masked_score)
    new_max = jnp.maximum(row_max, jnp.max(scores, axis=-1))
    weights = jnp.exp(scores - new_max[..., None])
    factor = jnp.exp(row_max - new_max)
    new_sum = row_sum * factor + jnp.sum(weights, axis=-1)
    update = jnp.einsum(
        "agts,sad->agtd",
        weights.astype(jnp.bfloat16),
        value_heads,
        preferred_element_type=jnp.float32,
    )
    return (new_max, new_sum, accum * factor[..., None] + update)


def on_device(queries, keys, values, segments, out_weight):
    row_count = queries.shape[0]
    kv_width = keys.shape[1]
    kv_heads = kv_width // HD
    group_size = queries.shape[1] // kv_width
    cycle_size = lax.axis_size("seq")
    position = lax.axis_index("seq")
    window_len = WIN_BLK * row_count
    reach_blocks = min(WIN_BLK, cycle_size - 1)
    own_first = position * row_count
    query_pos = own_first + jnp.arange(row_count, dtype=jnp.int32)
    query_seg = lax.dynamic_slice_in_dim(segments, own_first, row_count, 0)
    query_heads = queries.reshape(row_count, kv_heads, group_size, HD)
    start_state = (
        jnp.full((kv_heads, group_size, row_count), masked_score, jnp.float32),
        jnp.zeros((kv_heads, group_size, row_count), jnp.float32),
        jnp.zeros((kv_heads, group_size, row_count, HD), jnp.float32),
    )

    def take_block(carry_state, key_piece, value_piece, key_first):
        allowed = allowed_keys(
            segments, query_pos, query_seg, key_first, key_piece.shape[0], window_len
        )
        return absorb(carry_state, query_heads, key_piece, value_piece, allowed)

    carry_state = take_block(start_state, keys, values, own_first)
    near_keys, near_values = passed_along((keys, values), "seq", 1)
    carry_state = take_block(carry_state, near_keys, near_values, own_first - row_count)
    pair_keys = jnp.concatenate([near_keys, keys], axis=0)
    pair_values = jnp.concatenate([near_values, values], axis=0)

    def pair_turn(turn_index, loop_carry):
        moving_keys, moving_values, inner_state = loop_carry
        moving_keys, moving_values = passed_along((moving_keys, moving_values), "seq", 2)
        key_first = own_first - (2 * turn_index + 3) * row_count
        inner_state = take_block(inner_state, moving_keys, moving_values, key_first)
        return (moving_keys, moving_values, inner_state)

    finished = lax.fori_loop(0, reach_blocks // 2, pair_turn, (pair_keys, pair_values, carry_state))
    carry_state = finished[2]
    row_max, row_sum, accum = carry_state
    attended = (accum / row_sum[..., None]).transpose(2, 0, 1, 3)
    attended = attended.reshape(row_count, queries.shape[1]).astype(jnp.bfloat16)
    mixed = jnp.dot(
        lax.all_gather(attended, "head", axis=1, tiled=True),
        out_weight,
        preferred_element_type=jnp.float32,
    )
    return mixed.astype(jnp.bfloat16)


SUBTILE = 16
MAX_REACH = 3
PAIRS = 2


def needed_reach(token_count, row_count, cycle_size):
    back = token_count // 3 - 1
    return min(WIN_BLK, cycle_size - 1, -(-back // row_count))


def fused_kernel(
    reach, far_rows, cycle_size, q_hbm, k_hbm, v_hbm, seg_hbm, w_hbm, out_ref,
    q_ref, kv_ref, seg_ref, w_ref, att_ref, acc_ref,
    load_sem, w_sem, kv_send, kv_recv, att_send, att_recv,
):
    rows = k_hbm.shape[0]
    width = q_hbm.shape[1]
    group = width // HD
    pair_width = width // PAIRS
    seq = lax.axis_index("seq")
    head = lax.axis_index("head")
    x_at, y_at = head % 2, head // 2
    peers = (head, head + 1 - 2 * x_at, head + 2 - 4 * y_at, 3 - head)
    own_at = reach * rows

    barrier = pltpu.get_barrier_semaphore()
    for peer in peers[1:]:
        pl.semaphore_signal(barrier, inc=1, device_id={"head": peer})
    for d in range(1, reach + 1):
        @pl.when(seq + d < cycle_size)
        def _():
            pl.semaphore_signal(barrier, inc=1, device_id={"seq": seq + d})

        @pl.when(seq - d >= 0)
        def _():
            pl.semaphore_signal(barrier, inc=1, device_id={"seq": seq - d})

    own = [
        pltpu.make_async_copy(src, kv_ref.at[i, pl.ds(own_at, rows), :], load_sem.at[i])
        for i, src in enumerate((k_hbm, v_hbm))
    ]
    q_load = pltpu.make_async_copy(q_hbm, q_ref, load_sem.at[2])
    seg_load = pltpu.make_async_copy(seg_hbm, seg_ref, load_sem.at[3])
    for copy in own + [q_load, seg_load]:
        copy.start()
    w_loads = []
    for r, peer in enumerate(peers):
        first = pl.multiple_of(peer * width, width)
        w_loads.append(pltpu.make_async_copy(w_hbm.at[pl.ds(first, width), :], w_ref.at[r], w_sem.at[r]))
        w_loads[r].start()

    def kv_copy(d, i):
        skip = rows - far_rows if d == reach else 0
        return pltpu.make_async_remote_copy(
            src_ref=kv_ref.at[i, pl.ds(own_at + skip, rows - skip), :],
            dst_ref=kv_ref.at[i, pl.ds(own_at - d * rows + skip, rows - skip), :],
            send_sem=kv_send.at[d - 1, i],
            recv_sem=kv_recv.at[d - 1, i],
            device_id={"seq": seq + d},
        )

    if far_rows < rows:
        kv_ref[:, : rows - far_rows, :] = jnp.zeros((2, rows - far_rows, HD), jnp.bfloat16)
    for d in range(1, reach + 1):
        skip = rows - far_rows if d == reach else 0

        @pl.when(seq - d < 0)
        def _():
            kv_ref[:, pl.ds(own_at - d * rows + skip, rows - skip), :] = jnp.zeros(
                (2, rows - skip, HD), jnp.bfloat16)

    greeted = 3 + jnp.minimum(seq, reach) + jnp.minimum(cycle_size - 1 - seq, reach)
    pl.semaphore_wait(barrier, greeted)

    for i in range(2):
        own[i].wait()
        for d in range(reach, 0, -1):
            @pl.when(seq + d < cycle_size)
            def _():
                kv_copy(d, i).start()

    seg_load.wait()
    length = (reach + 1) * rows
    key_seg = jnp.concatenate(
        [seg_ref[pl.ds((seq - d + cycle_size) % cycle_size, 1), :] for d in range(reach, -1, -1)], axis=1)
    seg_own = seg_ref[pl.ds(seq, 1), :]
    query_seg = jnp.broadcast_to(seg_own, (rows, rows)).T
    query_seg = jnp.concatenate([query_seg] * (reach + 1), axis=1)
    query_pos = seq * rows + lax.broadcasted_iota(jnp.int32, (rows, length), 0)
    key_pos = (seq - reach) * rows + lax.broadcasted_iota(jnp.int32, (rows, length), 1)
    allowed = (key_pos <= query_pos) & (query_pos - key_pos < WIN_BLK * rows) & (key_pos >= 0)
    allowed = allowed & (key_seg == query_seg)

    q_load.wait()

    def arrivals(i):
        for d in range(1, reach + 1):
            @pl.when(seq - d >= 0)
            def _():
                kv_copy(d, i).wait_recv()

    arrivals(0)
    arrivals(1)
    factor = HD ** (-0.5) * math.log2(math.e)

    def att_copy(r, c):
        return pltpu.make_async_remote_copy(
            src_ref=att_ref.at[0, c],
            dst_ref=att_ref.at[r, c],
            send_sem=att_send.at[r - 1, c],
            recv_sem=att_recv.at[r - 1, c],
            device_id={"head": peers[r]},
        )

    per_pair = group // PAIRS
    for h in range(group):
        q_h = q_ref[:, h * HD:(h + 1) * HD]
        scores = lax.dot_general(
            q_h, kv_ref[0], (((1,), (1,)), ((), ())), preferred_element_type=jnp.float32)
        scores = jnp.where(allowed, scores, masked_score)
        row_max = jnp.max(scores, axis=1, keepdims=True)
        raw = jnp.exp2((scores - row_max) * factor)
        total = jnp.sum(raw, axis=1, keepdims=True)
        part = jnp.dot(raw.astype(jnp.bfloat16), kv_ref[1], preferred_element_type=jnp.float32)
        c, place = h // per_pair, h % per_pair
        att_ref[0, c, :, place * HD:(place + 1) * HD] = (part / total).astype(jnp.bfloat16)
        if place == per_pair - 1:
            for r in (3, 1, 2):
                att_copy(r, c).start()

    order = [(0, 0), (0, 1)] + [(r, c) for c in range(PAIRS) for r in (1, 2, 3)]
    for step, (r, c) in enumerate(order):
        if r:
            att_copy(r, c).wait_recv()
        if c == 0:
            w_loads[r].wait()
        piece = jnp.dot(
            att_ref[r, c], w_ref[r, c * pair_width:(c + 1) * pair_width, :],
            preferred_element_type=jnp.float32)
        if step == 0:
            acc_ref[...] = piece
        elif step < len(order) - 1:
            acc_ref[...] += piece
        else:
            out_ref[...] = (acc_ref[...] + piece).astype(jnp.bfloat16)

    for d in range(1, reach + 1):
        @pl.when(seq + d < cycle_size)
        def _():
            kv_copy(d, 0).wait_send()
            kv_copy(d, 1).wait_send()
    for r in range(1, 4):
        for c in range(PAIRS):
            att_copy(r, c).wait_send()


def fused(reach, queries, keys, values, segments, out_weight):
    rows, width = queries.shape
    cycle_size = lax.axis_size("seq")
    features = out_weight.shape[1]
    back = segments.shape[0] // 3 - 1 - (reach - 1) * rows
    far_rows = min(rows, -(-back // SUBTILE) * SUBTILE)
    any_spec = pl.BlockSpec(memory_space=pl.ANY)
    pair_width = width // PAIRS
    return pl.pallas_call(
        functools.partial(fused_kernel, reach, far_rows, cycle_size),
        out_shape=jax.ShapeDtypeStruct((rows, features), jnp.bfloat16),
        in_specs=[any_spec] * 5,
        out_specs=pl.BlockSpec(memory_space=pltpu.VMEM),
        scratch_shapes=[
            pltpu.VMEM((rows, width), jnp.bfloat16),
            pltpu.VMEM((2, (reach + 1) * rows, HD), jnp.bfloat16),
            pltpu.VMEM((cycle_size, rows), jnp.int32),
            pltpu.VMEM((4, width, features), jnp.bfloat16),
            pltpu.VMEM((4, PAIRS, rows, pair_width), jnp.bfloat16),
            pltpu.VMEM((rows, features), jnp.float32),
            pltpu.SemaphoreType.DMA((4,)),
            pltpu.SemaphoreType.DMA((4,)),
            pltpu.SemaphoreType.DMA((reach, 2)),
            pltpu.SemaphoreType.DMA((reach, 2)),
            pltpu.SemaphoreType.DMA((3, PAIRS)),
            pltpu.SemaphoreType.DMA((3, PAIRS)),
        ],
        compiler_params=pltpu.CompilerParams(collective_id=0, has_side_effects=True),
    )(queries, keys, values, segments.reshape(cycle_size, rows), out_weight)


def chosen(queries, keys, values, segments, out_weight):
    row_count, width = queries.shape
    cycle_size = lax.axis_size("seq")
    reach = needed_reach(segments.shape[0], row_count, cycle_size)
    fits = 1 <= reach <= MAX_REACH and lax.axis_size("head") == 4
    fits = fits and keys.shape[1] == HD and width % (PAIRS * HD) == 0
    if fits and row_count == HD and 4 * width == out_weight.shape[0]:
        return fused(reach, queries, keys, values, segments, out_weight)
    return on_device(queries, keys, values, segments, out_weight)


def solution(mesh):
    return jax.shard_map(
        chosen,
        mesh=mesh,
        in_specs=(P("seq", "head"), P("seq", "head"), P("seq", "head"), P(), P(None, "head")),
        out_specs=P("seq", "head"),
        check_vma=False,
    )
```

```python
import functools
import math

import jax
import jax.numpy as jnp
from jax import lax
from jax.experimental import pallas as pl
from jax.experimental.pallas import tpu as pltpu
from jax.sharding import PartitionSpec as P

HD = 128
WIN_BLK = 31


masked_score = -1e30


def passed_along(block, axis, distance):
    devices = range(lax.axis_size(axis))
    route = [(i - distance, i) for i in devices if i - distance in devices]
    return lax.ppermute(block, axis, route)


def allowed_keys(segments, query_pos, query_seg, key_first, key_count, window_len):
    key_pos = key_first + jnp.arange(key_count, dtype=jnp.int32)
    clipped = jnp.clip(key_pos, 0, segments.shape[0] - 1)
    key_seg = jnp.take(segments, clipped)
    allowed = key_pos[None, :] <= query_pos[:, None]
    allowed = allowed & (query_pos[:, None] - key_pos[None, :] < window_len)
    allowed = allowed & (key_pos[None, :] >= 0)
    return allowed & (key_seg[None, :] == query_seg[:, None])


def absorb(carry_state, query_heads, key_piece, value_piece, allowed):
    row_max, row_sum, accum = carry_state
    key_count = key_piece.shape[0]
    kv_heads = query_heads.shape[1]
    key_heads = key_piece.reshape(key_count, kv_heads, HD)
    value_heads = value_piece.reshape(key_count, kv_heads, HD)
    scores = jnp.einsum(
        "tagd,sad->agts", query_heads, key_heads, preferred_element_type=jnp.float32
    )
    scores = jnp.where(allowed[None, None], scores * HD ** (-0.5), masked_score)
    new_max = jnp.maximum(row_max, jnp.max(scores, axis=-1))
    weights = jnp.exp(scores - new_max[..., None])
    factor = jnp.exp(row_max - new_max)
    new_sum = row_sum * factor + jnp.sum(weights, axis=-1)
    update = jnp.einsum(
        "agts,sad->agtd",
        weights.astype(jnp.bfloat16),
        value_heads,
        preferred_element_type=jnp.float32,
    )
    return (new_max, new_sum, accum * factor[..., None] + update)


def on_device(queries, keys, values, segments, out_weight):
    row_count = queries.shape[0]
    kv_width = keys.shape[1]
    kv_heads = kv_width // HD
    group_size = queries.shape[1] // kv_width
    cycle_size = lax.axis_size("seq")
    position = lax.axis_index("seq")
    window_len = WIN_BLK * row_count
    reach_blocks = min(WIN_BLK, cycle_size - 1)
    own_first = position * row_count
    query_pos = own_first + jnp.arange(row_count, dtype=jnp.int32)
    query_seg = lax.dynamic_slice_in_dim(segments, own_first, row_count, 0)
    query_heads = queries.reshape(row_count, kv_heads, group_size, HD)
    start_state = (
        jnp.full((kv_heads, group_size, row_count), masked_score, jnp.float32),
        jnp.zeros((kv_heads, group_size, row_count), jnp.float32),
        jnp.zeros((kv_heads, group_size, row_count, HD), jnp.float32),
    )

    def take_block(carry_state, key_piece, value_piece, key_first):
        allowed = allowed_keys(
            segments, query_pos, query_seg, key_first, key_piece.shape[0], window_len
        )
        return absorb(carry_state, query_heads, key_piece, value_piece, allowed)

    carry_state = take_block(start_state, keys, values, own_first)
    near_keys, near_values = passed_along((keys, values), "seq", 1)
    carry_state = take_block(carry_state, near_keys, near_values, own_first - row_count)
    pair_keys = jnp.concatenate([near_keys, keys], axis=0)
    pair_values = jnp.concatenate([near_values, values], axis=0)

    def pair_turn(turn_index, loop_carry):
        moving_keys, moving_values, inner_state = loop_carry
        moving_keys, moving_values = passed_along((moving_keys, moving_values), "seq", 2)
        key_first = own_first - (2 * turn_index + 3) * row_count
        inner_state = take_block(inner_state, moving_keys, moving_values, key_first)
        return (moving_keys, moving_values, inner_state)

    finished = lax.fori_loop(0, reach_blocks // 2, pair_turn, (pair_keys, pair_values, carry_state))
    carry_state = finished[2]
    row_max, row_sum, accum = carry_state
    attended = (accum / row_sum[..., None]).transpose(2, 0, 1, 3)
    attended = attended.reshape(row_count, queries.shape[1]).astype(jnp.bfloat16)
    mixed = jnp.dot(
        lax.all_gather(attended, "head", axis=1, tiled=True),
        out_weight,
        preferred_element_type=jnp.float32,
    )
    return mixed.astype(jnp.bfloat16)


SUBTILE = 16
MAX_REACH = 3
PAIRS = 2
VMEM_GRANT = 32 * 2**20


def needed_reach(token_count, row_count, cycle_size):
    back = token_count // 3 - 1
    return min(WIN_BLK, cycle_size - 1, -(-back // row_count))


def fused_kernel(
    reach, far_rows, cycle_size, q_hbm, k_hbm, v_hbm, seg_hbm, w_hbm, out_ref,
    q_ref, kv_ref, seg_ref, w_ref, att_ref, acc_ref,
    load_sem, w_sem, kv_send, kv_recv, att_send, att_recv,
):
    rows = k_hbm.shape[0]
    width = q_hbm.shape[1]
    group = width // HD
    pair_width = width // PAIRS
    seq = lax.axis_index("seq")
    head = lax.axis_index("head")
    x_at, y_at = head % 2, head // 2
    peers = (head, head + 1 - 2 * x_at, head + 2 - 4 * y_at, 3 - head)
    own_at = reach * rows

    barrier = pltpu.get_barrier_semaphore()
    for peer in peers[1:]:
        pl.semaphore_signal(barrier, inc=1, device_id={"head": peer})
    for d in range(1, reach + 1):
        @pl.when(seq + d < cycle_size)
        def _():
            pl.semaphore_signal(barrier, inc=1, device_id={"seq": seq + d})

        @pl.when(seq - d >= 0)
        def _():
            pl.semaphore_signal(barrier, inc=1, device_id={"seq": seq - d})

    own = [
        pltpu.make_async_copy(src, kv_ref.at[i, pl.ds(own_at, rows), :], load_sem.at[i])
        for i, src in enumerate((k_hbm, v_hbm))
    ]
    q_load = pltpu.make_async_copy(q_hbm, q_ref, load_sem.at[2])
    seg_load = pltpu.make_async_copy(seg_hbm, seg_ref, load_sem.at[3])
    for copy in own + [q_load, seg_load]:
        copy.start()
    w_loads = []
    for r, peer in enumerate(peers):
        first = pl.multiple_of(peer * width, width)
        w_loads.append(pltpu.make_async_copy(w_hbm.at[pl.ds(first, width), :], w_ref.at[r], w_sem.at[r]))
        w_loads[r].start()

    def kv_copy(d, i):
        skip = rows - far_rows if d == reach else 0
        return pltpu.make_async_remote_copy(
            src_ref=kv_ref.at[i, pl.ds(own_at + skip, rows - skip), :],
            dst_ref=kv_ref.at[i, pl.ds(own_at - d * rows + skip, rows - skip), :],
            send_sem=kv_send.at[d - 1, i],
            recv_sem=kv_recv.at[d - 1, i],
            device_id={"seq": seq + d},
        )

    if far_rows < rows:
        kv_ref[:, : rows - far_rows, :] = jnp.zeros((2, rows - far_rows, HD), jnp.bfloat16)
    for d in range(1, reach + 1):
        skip = rows - far_rows if d == reach else 0

        @pl.when(seq - d < 0)
        def _():
            kv_ref[:, pl.ds(own_at - d * rows + skip, rows - skip), :] = jnp.zeros(
                (2, rows - skip, HD), jnp.bfloat16)

    greeted = 3 + jnp.minimum(seq, reach) + jnp.minimum(cycle_size - 1 - seq, reach)
    pl.semaphore_wait(barrier, greeted)

    for i in range(2):
        own[i].wait()
        for d in range(reach, 0, -1):
            @pl.when(seq + d < cycle_size)
            def _():
                kv_copy(d, i).start()

    seg_load.wait()
    length = (reach + 1) * rows
    key_seg = jnp.concatenate(
        [seg_ref[pl.ds((seq - d + cycle_size) % cycle_size, 1), :] for d in range(reach, -1, -1)], axis=1)
    seg_own = seg_ref[pl.ds(seq, 1), :]
    query_seg = jnp.broadcast_to(seg_own, (rows, rows)).T
    query_seg = jnp.concatenate([query_seg] * (reach + 1), axis=1)
    query_pos = seq * rows + lax.broadcasted_iota(jnp.int32, (rows, length), 0)
    key_pos = (seq - reach) * rows + lax.broadcasted_iota(jnp.int32, (rows, length), 1)
    allowed = (key_pos <= query_pos) & (query_pos - key_pos < WIN_BLK * rows) & (key_pos >= 0)
    allowed = allowed & (key_seg == query_seg)

    q_load.wait()

    def arrivals(i):
        for d in range(1, reach + 1):
            @pl.when(seq - d >= 0)
            def _():
                kv_copy(d, i).wait_recv()

    arrivals(0)
    arrivals(1)
    factor = HD ** (-0.5) * math.log2(math.e)

    def att_copy(r, c):
        return pltpu.make_async_remote_copy(
            src_ref=att_ref.at[0, c],
            dst_ref=att_ref.at[r, c],
            send_sem=att_send.at[r - 1, c],
            recv_sem=att_recv.at[r - 1, c],
            device_id={"head": peers[r]},
        )

    per_pair = group // PAIRS
    for h in range(group):
        q_h = q_ref[:, h * HD:(h + 1) * HD]
        scores = lax.dot_general(
            q_h, kv_ref[0], (((1,), (1,)), ((), ())), preferred_element_type=jnp.float32)
        scores = jnp.where(allowed, scores, masked_score)
        row_max = jnp.max(scores, axis=1, keepdims=True)
        raw = jnp.exp2((scores - row_max) * factor)
        total = jnp.sum(raw, axis=1, keepdims=True)
        part = jnp.dot(raw.astype(jnp.bfloat16), kv_ref[1], preferred_element_type=jnp.float32)
        c, place = h // per_pair, h % per_pair
        att_ref[0, c, :, place * HD:(place + 1) * HD] = (part / total).astype(jnp.bfloat16)
        if place == per_pair - 1:
            for r in (3, 1, 2):
                att_copy(r, c).start()

    order = [(0, 0), (0, 1)] + [(r, c) for c in range(PAIRS) for r in (1, 2, 3)]
    for step, (r, c) in enumerate(order):
        if r:
            att_copy(r, c).wait_recv()
        if c == 0:
            w_loads[r].wait()
        piece = jnp.dot(
            att_ref[r, c], w_ref[r, c * pair_width:(c + 1) * pair_width, :],
            preferred_element_type=jnp.float32)
        if step == 0:
            acc_ref[...] = piece
        elif step < len(order) - 1:
            acc_ref[...] += piece
        else:
            out_ref[...] = (acc_ref[...] + piece).astype(jnp.bfloat16)

    for d in range(1, reach + 1):
        @pl.when(seq + d < cycle_size)
        def _():
            kv_copy(d, 0).wait_send()
            kv_copy(d, 1).wait_send()
    for r in range(1, 4):
        for c in range(PAIRS):
            att_copy(r, c).wait_send()


def fused(reach, queries, keys, values, segments, out_weight):
    rows, width = queries.shape
    cycle_size = lax.axis_size("seq")
    features = out_weight.shape[1]
    back = segments.shape[0] // 3 - 1 - (reach - 1) * rows
    far_rows = min(rows, -(-back // SUBTILE) * SUBTILE)
    hbm_spec = pl.BlockSpec(memory_space=pltpu.HBM)
    pair_width = width // PAIRS
    operands = (queries, keys, values, segments.reshape(cycle_size, rows), out_weight)
    return pl.pallas_call(
        functools.partial(fused_kernel, reach, far_rows, cycle_size),
        out_shape=pltpu.VMEM((rows, features), jnp.bfloat16),
        in_specs=[hbm_spec] * 5,
        out_specs=pl.BlockSpec(memory_space=pltpu.VMEM),
        scratch_shapes=[
            pltpu.VMEM((rows, width), jnp.bfloat16),
            pltpu.VMEM((2, (reach + 1) * rows, HD), jnp.bfloat16),
            pltpu.VMEM((cycle_size, rows), jnp.int32),
            pltpu.VMEM((4, width, features), jnp.bfloat16),
            pltpu.VMEM((4, PAIRS, rows, pair_width), jnp.bfloat16),
            pltpu.VMEM((rows, features), jnp.float32),
            pltpu.SemaphoreType.DMA((4,)),
            pltpu.SemaphoreType.DMA((4,)),
            pltpu.SemaphoreType.DMA((reach, 2)),
            pltpu.SemaphoreType.DMA((reach, 2)),
            pltpu.SemaphoreType.DMA((3, PAIRS)),
            pltpu.SemaphoreType.DMA((3, PAIRS)),
        ],
        compiler_params=pltpu.CompilerParams(
            collective_id=0, has_side_effects=True, vmem_limit_bytes=VMEM_GRANT),
    )(*(pltpu.with_memory_space_constraint(a, pltpu.HBM) for a in operands))


def chosen(queries, keys, values, segments, out_weight):
    row_count, width = queries.shape
    cycle_size = lax.axis_size("seq")
    reach = needed_reach(segments.shape[0], row_count, cycle_size)
    fits = 1 <= reach <= MAX_REACH and lax.axis_size("head") == 4
    fits = fits and keys.shape[1] == HD and width % (PAIRS * HD) == 0
    if fits and row_count == HD and 4 * width == out_weight.shape[0]:
        return fused(reach, queries, keys, values, segments, out_weight)
    return on_device(queries, keys, values, segments, out_weight)


def solution(mesh):
    return jax.shard_map(
        chosen,
        mesh=mesh,
        in_specs=(P("seq", "head"), P("seq", "head"), P("seq", "head"), P(), P(None, "head")),
        out_specs=P("seq", "head"),
        check_vma=False,
    )
```

```python
import functools
import math

import jax
import jax.numpy as jnp
from jax import lax
from jax.experimental import pallas as pl
from jax.experimental.pallas import tpu as pltpu
from jax.sharding import PartitionSpec as P

HD = 128
WIN_BLK = 31


masked_score = -1e30


def passed_along(block, axis, distance):
    devices = range(lax.axis_size(axis))
    route = [(i - distance, i) for i in devices if i - distance in devices]
    return lax.ppermute(block, axis, route)


def allowed_keys(segments, query_pos, query_seg, key_first, key_count, window_len):
    key_pos = key_first + jnp.arange(key_count, dtype=jnp.int32)
    clipped = jnp.clip(key_pos, 0, segments.shape[0] - 1)
    key_seg = jnp.take(segments, clipped)
    allowed = key_pos[None, :] <= query_pos[:, None]
    allowed = allowed & (query_pos[:, None] - key_pos[None, :] < window_len)
    allowed = allowed & (key_pos[None, :] >= 0)
    return allowed & (key_seg[None, :] == query_seg[:, None])


def absorb(carry_state, query_heads, key_piece, value_piece, allowed):
    row_max, row_sum, accum = carry_state
    key_count = key_piece.shape[0]
    kv_heads = query_heads.shape[1]
    key_heads = key_piece.reshape(key_count, kv_heads, HD)
    value_heads = value_piece.reshape(key_count, kv_heads, HD)
    scores = jnp.einsum(
        "tagd,sad->agts", query_heads, key_heads, preferred_element_type=jnp.float32
    )
    scores = jnp.where(allowed[None, None], scores * HD ** (-0.5), masked_score)
    new_max = jnp.maximum(row_max, jnp.max(scores, axis=-1))
    weights = jnp.exp(scores - new_max[..., None])
    factor = jnp.exp(row_max - new_max)
    new_sum = row_sum * factor + jnp.sum(weights, axis=-1)
    update = jnp.einsum(
        "agts,sad->agtd",
        weights.astype(jnp.bfloat16),
        value_heads,
        preferred_element_type=jnp.float32,
    )
    return (new_max, new_sum, accum * factor[..., None] + update)


def on_device(queries, keys, values, segments, out_weight):
    row_count = queries.shape[0]
    kv_width = keys.shape[1]
    kv_heads = kv_width // HD
    group_size = queries.shape[1] // kv_width
    cycle_size = lax.axis_size("seq")
    position = lax.axis_index("seq")
    window_len = WIN_BLK * row_count
    reach_blocks = min(WIN_BLK, cycle_size - 1)
    own_first = position * row_count
    query_pos = own_first + jnp.arange(row_count, dtype=jnp.int32)
    query_seg = lax.dynamic_slice_in_dim(segments, own_first, row_count, 0)
    query_heads = queries.reshape(row_count, kv_heads, group_size, HD)
    start_state = (
        jnp.full((kv_heads, group_size, row_count), masked_score, jnp.float32),
        jnp.zeros((kv_heads, group_size, row_count), jnp.float32),
        jnp.zeros((kv_heads, group_size, row_count, HD), jnp.float32),
    )

    def take_block(carry_state, key_piece, value_piece, key_first):
        allowed = allowed_keys(
            segments, query_pos, query_seg, key_first, key_piece.shape[0], window_len
        )
        return absorb(carry_state, query_heads, key_piece, value_piece, allowed)

    carry_state = take_block(start_state, keys, values, own_first)
    near_keys, near_values = passed_along((keys, values), "seq", 1)
    carry_state = take_block(carry_state, near_keys, near_values, own_first - row_count)
    pair_keys = jnp.concatenate([near_keys, keys], axis=0)
    pair_values = jnp.concatenate([near_values, values], axis=0)

    def pair_turn(turn_index, loop_carry):
        moving_keys, moving_values, inner_state = loop_carry
        moving_keys, moving_values = passed_along((moving_keys, moving_values), "seq", 2)
        key_first = own_first - (2 * turn_index + 3) * row_count
        inner_state = take_block(inner_state, moving_keys, moving_values, key_first)
        return (moving_keys, moving_values, inner_state)

    finished = lax.fori_loop(0, reach_blocks // 2, pair_turn, (pair_keys, pair_values, carry_state))
    carry_state = finished[2]
    row_max, row_sum, accum = carry_state
    attended = (accum / row_sum[..., None]).transpose(2, 0, 1, 3)
    attended = attended.reshape(row_count, queries.shape[1]).astype(jnp.bfloat16)
    mixed = jnp.dot(
        lax.all_gather(attended, "head", axis=1, tiled=True),
        out_weight,
        preferred_element_type=jnp.float32,
    )
    return mixed.astype(jnp.bfloat16)


SUBTILE = 16
REACH = 3
PAIRS = 2
VMEM_GRANT = 32 * 2**20


def needed_reach(token_count, row_count, cycle_size):
    back = token_count // 3 - 1
    return min(WIN_BLK, cycle_size - 1, -(-back // row_count))


def fused_kernel(
    reach, far_rows, cycle_size, q_hbm, k_hbm, v_hbm, seg_hbm, w_hbm, out_ref,
    q_ref, kv_ref, seg_ref, w_ref, att_ref, acc_ref,
    load_sem, w_sem, kv_send, kv_recv, att_send, att_recv,
):
    rows = k_hbm.shape[0]
    width = q_hbm.shape[1]
    group = width // HD
    pair_width = width // PAIRS
    seq = lax.axis_index("seq")
    head = lax.axis_index("head")
    x_at, y_at = head % 2, head // 2
    peers = (head, head + 1 - 2 * x_at, head + 2 - 4 * y_at, 3 - head)
    own_at = reach * rows

    core = seq % 2
    partner = seq + 1 - 2 * core
    has_next, has_last = seq + 2 < cycle_size, seq - 2 >= 0
    sends_far = (core == 1) & (seq + 3 < cycle_size)
    takes_far = (core == 0) & (seq - 3 >= 0)

    barrier = pltpu.get_barrier_semaphore()

    def greet(axis, place):
        pl.semaphore_signal(barrier, inc=1, device_id={axis: place})

    pl.when(has_next)(lambda: greet("seq", seq + 2))
    pl.when(has_last)(lambda: greet("seq", seq - 2))
    pl.when(sends_far)(lambda: greet("seq", seq + 3))
    pl.when(takes_far)(lambda: greet("seq", seq - 3))
    greet("head", peers[1])
    greet("head", peers[2])
    greet("seq", partner)

    own = [
        pltpu.make_async_copy(src, kv_ref.at[i, pl.ds(own_at, rows), :], load_sem.at[i])
        for i, src in enumerate((k_hbm, v_hbm))
    ]
    q_load = pltpu.make_async_copy(q_hbm, q_ref, load_sem.at[2])
    seg_load = pltpu.make_async_copy(seg_hbm, seg_ref, load_sem.at[3])
    for copy in own + [q_load, seg_load]:
        copy.start()
    w_loads = []
    for r, peer in enumerate(peers):
        first = pl.multiple_of(peer * width, width)
        w_loads.append(pltpu.make_async_copy(w_hbm.at[pl.ds(first, width), :], w_ref.at[r], w_sem.at[r]))
        w_loads[r].start()

    def kv_copy(held, d, i, target):
        skip = rows - far_rows if d == reach else 0
        return pltpu.make_async_remote_copy(
            src_ref=kv_ref.at[i, pl.ds(own_at - held * rows + skip, rows - skip), :],
            dst_ref=kv_ref.at[i, pl.ds(own_at - d * rows + skip, rows - skip), :],
            send_sem=kv_send.at[d - 1, i],
            recv_sem=kv_recv.at[d - 1, i],
            device_id={"seq": target},
        )

    if far_rows < rows:
        kv_ref[:, : rows - far_rows, :] = jnp.zeros((2, rows - far_rows, HD), jnp.bfloat16)
    for d in range(1, reach + 1):
        skip = rows - far_rows if d == reach else 0

        @pl.when(seq - d < 0)
        def _():
            kv_ref[:, pl.ds(own_at - d * rows + skip, rows - skip), :] = jnp.zeros(
                (2, rows - skip, HD), jnp.bfloat16)

    far_peer = core * jnp.minimum(1, (cycle_size - 1 - seq) // 3) + (1 - core) * jnp.minimum(1, seq // 3)
    near_peers = jnp.minimum(1, (cycle_size - 1 - seq) // 2) + jnp.minimum(1, seq // 2)
    pl.semaphore_wait(barrier, 3 + near_peers + far_peer)

    for i in range(2):
        own[i].wait()
        pl.when(has_next)(lambda i=i: kv_copy(0, 2, i, seq + 2).start())
        pl.when(sends_far)(lambda i=i: kv_copy(0, 3, i, seq + 3).start())
        pl.when(core == 0)(lambda i=i: kv_copy(0, 1, i, partner).start())

    seg_load.wait()
    length = (reach + 1) * rows
    key_seg = jnp.concatenate(
        [seg_ref[pl.ds((seq - d + cycle_size) % cycle_size, 1), :] for d in range(reach, -1, -1)], axis=1)
    seg_own = seg_ref[pl.ds(seq, 1), :]
    query_seg = jnp.broadcast_to(seg_own, (rows, rows)).T
    query_seg = jnp.concatenate([query_seg] * (reach + 1), axis=1)
    query_pos = seq * rows + lax.broadcasted_iota(jnp.int32, (rows, length), 0)
    key_pos = (seq - reach) * rows + lax.broadcasted_iota(jnp.int32, (rows, length), 1)
    allowed = (key_pos <= query_pos) & (query_pos - key_pos < WIN_BLK * rows) & (key_pos >= 0)
    allowed = allowed & (key_seg == query_seg)

    q_load.wait()

    def relay(i):
        @pl.when(has_last)
        def _():
            kv_copy(0, 2, i, partner).wait_recv()

            @pl.when(core == 0)
            def _():
                kv_copy(2, 3, i, partner).start()

            @pl.when(core == 1)
            def _():
                kv_copy(2, 1, i, partner).start()

    def arrivals(i):
        pl.when((core == 1) | has_last)(lambda: kv_copy(0, 1, i, partner).wait_recv())
        pl.when(((core == 1) & has_last) | takes_far)(lambda: kv_copy(0, 3, i, partner).wait_recv())

    relay(0)
    relay(1)
    arrivals(0)
    factor = HD ** (-0.5) * math.log2(math.e)

    def att_copy(held, r, c, target):
        return pltpu.make_async_remote_copy(
            src_ref=att_ref.at[held, c],
            dst_ref=att_ref.at[r, c],
            send_sem=att_send.at[r - 1, c],
            recv_sem=att_recv.at[r - 1, c],
            device_id={"head": peers[target]},
        )

    per_pair = group // PAIRS
    probs, totals = [], []
    for h in range(group):
        q_h = q_ref[:, h * HD:(h + 1) * HD]
        scores = lax.dot_general(
            q_h, kv_ref[0], (((1,), (1,)), ((), ())), preferred_element_type=jnp.float32)
        scores = jnp.where(allowed, scores, masked_score)
        row_max = jnp.max(scores, axis=1, keepdims=True)
        raw = jnp.exp2((scores - row_max) * factor)
        totals.append(jnp.sum(raw, axis=1, keepdims=True))
        probs.append(raw.astype(jnp.bfloat16))
    arrivals(1)
    for h in range(group):
        part = jnp.dot(probs[h], kv_ref[1], preferred_element_type=jnp.float32)
        c, place = h // per_pair, h % per_pair
        att_ref[0, c, :, place * HD:(place + 1) * HD] = (part / totals[h]).astype(jnp.bfloat16)
        if h == per_pair - 1:
            att_copy(0, 1, 0, 1).start()
    att_copy(0, 2, 1, 2).start()
    att_copy(0, 1, 1, 1).start()
    att_copy(0, 2, 0, 2).start()

    order = [(0, 0), (0, 1), (1, 0), (2, 1), (1, 1), (2, 0), (3, 0), (3, 1)]
    loaded = set()
    for step, (r, c) in enumerate(order):
        if step == 2:
            att_copy(0, 1, 0, 1).wait_recv()
            att_copy(1, 3, 0, 2).start()
            att_copy(0, 2, 1, 2).wait_recv()
            att_copy(2, 3, 1, 1).start()
        elif step > 3:
            att_copy(0, r, c, 1).wait_recv()
        if r not in loaded:
            w_loads[r].wait()
            loaded.add(r)
        piece = jnp.dot(
            att_ref[r, c], w_ref[r, c * pair_width:(c + 1) * pair_width, :],
            preferred_element_type=jnp.float32)
        if step == 0:
            acc_ref[...] = piece
        elif step < len(order) - 1:
            acc_ref[...] += piece
        else:
            out_ref[...] = (acc_ref[...] + piece).astype(jnp.bfloat16)

    for i in range(2):
        pl.when(has_next)(lambda i=i: kv_copy(0, 2, i, seq + 2).wait_send())
        pl.when(sends_far | ((core == 0) & has_last))(lambda i=i: kv_copy(0, 3, i, partner).wait_send())
        pl.when((core == 0) | has_last)(lambda i=i: kv_copy(0, 1, i, partner).wait_send())
    for r in range(1, 4):
        for c in range(PAIRS):
            att_copy(0, r, c, 1).wait_send()


def fused(reach, queries, keys, values, segments, out_weight):
    rows, width = queries.shape
    cycle_size = lax.axis_size("seq")
    features = out_weight.shape[1]
    back = segments.shape[0] // 3 - 1 - (reach - 1) * rows
    far_rows = min(rows, -(-back // SUBTILE) * SUBTILE)
    hbm_spec = pl.BlockSpec(memory_space=pltpu.HBM)
    pair_width = width // PAIRS
    operands = (queries, keys, values, segments.reshape(cycle_size, rows), out_weight)
    return pl.pallas_call(
        functools.partial(fused_kernel, reach, far_rows, cycle_size),
        out_shape=pltpu.VMEM((rows, features), jnp.bfloat16),
        in_specs=[hbm_spec] * 5,
        out_specs=pl.BlockSpec(memory_space=pltpu.VMEM),
        scratch_shapes=[
            pltpu.VMEM((rows, width), jnp.bfloat16),
            pltpu.VMEM((2, (reach + 1) * rows, HD), jnp.bfloat16),
            pltpu.VMEM((cycle_size, rows), jnp.int32),
            pltpu.VMEM((4, width, features), jnp.bfloat16),
            pltpu.VMEM((4, PAIRS, rows, pair_width), jnp.bfloat16),
            pltpu.VMEM((rows, features), jnp.float32),
            pltpu.SemaphoreType.DMA((4,)),
            pltpu.SemaphoreType.DMA((4,)),
            pltpu.SemaphoreType.DMA((reach, 2)),
            pltpu.SemaphoreType.DMA((reach, 2)),
            pltpu.SemaphoreType.DMA((3, PAIRS)),
            pltpu.SemaphoreType.DMA((3, PAIRS)),
        ],
        compiler_params=pltpu.CompilerParams(
            collective_id=0, has_side_effects=True, vmem_limit_bytes=VMEM_GRANT),
    )(*(pltpu.with_memory_space_constraint(a, pltpu.HBM) for a in operands))


def chosen(queries, keys, values, segments, out_weight):
    row_count, width = queries.shape
    cycle_size = lax.axis_size("seq")
    reach = needed_reach(segments.shape[0], row_count, cycle_size)
    fits = reach == REACH and cycle_size % 2 == 0 and lax.axis_size("head") == 4
    fits = fits and keys.shape[1] == HD and width % (PAIRS * HD) == 0
    if fits and row_count == HD and 4 * width == out_weight.shape[0]:
        return fused(reach, queries, keys, values, segments, out_weight)
    return on_device(queries, keys, values, segments, out_weight)


def solution(mesh):
    return jax.shard_map(
        chosen,
        mesh=mesh,
        in_specs=(P("seq", "head"), P("seq", "head"), P("seq", "head"), P(), P(None, "head")),
        out_specs=P("seq", "head"),
        check_vma=False,
    )
```

```python
import functools
import math

import jax
import jax.numpy as jnp
from jax import lax
from jax.experimental import pallas as pl
from jax.experimental.pallas import tpu as pltpu
from jax.sharding import PartitionSpec as P

HD = 128
WIN_BLK = 31


masked_score = -1e30


def passed_along(block, axis, distance):
    devices = range(lax.axis_size(axis))
    route = [(i - distance, i) for i in devices if i - distance in devices]
    return lax.ppermute(block, axis, route)


def allowed_keys(segments, query_pos, query_seg, key_first, key_count, window_len):
    key_pos = key_first + jnp.arange(key_count, dtype=jnp.int32)
    clipped = jnp.clip(key_pos, 0, segments.shape[0] - 1)
    key_seg = jnp.take(segments, clipped)
    allowed = key_pos[None, :] <= query_pos[:, None]
    allowed = allowed & (query_pos[:, None] - key_pos[None, :] < window_len)
    allowed = allowed & (key_pos[None, :] >= 0)
    return allowed & (key_seg[None, :] == query_seg[:, None])


def absorb(carry_state, query_heads, key_piece, value_piece, allowed):
    row_max, row_sum, accum = carry_state
    key_count = key_piece.shape[0]
    kv_heads = query_heads.shape[1]
    key_heads = key_piece.reshape(key_count, kv_heads, HD)
    value_heads = value_piece.reshape(key_count, kv_heads, HD)
    scores = jnp.einsum(
        "tagd,sad->agts", query_heads, key_heads, preferred_element_type=jnp.float32
    )
    scores = jnp.where(allowed[None, None], scores * HD ** (-0.5), masked_score)
    new_max = jnp.maximum(row_max, jnp.max(scores, axis=-1))
    weights = jnp.exp(scores - new_max[..., None])
    factor = jnp.exp(row_max - new_max)
    new_sum = row_sum * factor + jnp.sum(weights, axis=-1)
    update = jnp.einsum(
        "agts,sad->agtd",
        weights.astype(jnp.bfloat16),
        value_heads,
        preferred_element_type=jnp.float32,
    )
    return (new_max, new_sum, accum * factor[..., None] + update)


def on_device(queries, keys, values, segments, out_weight):
    row_count = queries.shape[0]
    kv_width = keys.shape[1]
    kv_heads = kv_width // HD
    group_size = queries.shape[1] // kv_width
    cycle_size = lax.axis_size("seq")
    position = lax.axis_index("seq")
    window_len = WIN_BLK * row_count
    reach_blocks = min(WIN_BLK, cycle_size - 1)
    own_first = position * row_count
    query_pos = own_first + jnp.arange(row_count, dtype=jnp.int32)
    query_seg = lax.dynamic_slice_in_dim(segments, own_first, row_count, 0)
    query_heads = queries.reshape(row_count, kv_heads, group_size, HD)
    start_state = (
        jnp.full((kv_heads, group_size, row_count), masked_score, jnp.float32),
        jnp.zeros((kv_heads, group_size, row_count), jnp.float32),
        jnp.zeros((kv_heads, group_size, row_count, HD), jnp.float32),
    )

    def take_block(carry_state, key_piece, value_piece, key_first):
        allowed = allowed_keys(
            segments, query_pos, query_seg, key_first, key_piece.shape[0], window_len
        )
        return absorb(carry_state, query_heads, key_piece, value_piece, allowed)

    carry_state = take_block(start_state, keys, values, own_first)
    near_keys, near_values = passed_along((keys, values), "seq", 1)
    carry_state = take_block(carry_state, near_keys, near_values, own_first - row_count)
    pair_keys = jnp.concatenate([near_keys, keys], axis=0)
    pair_values = jnp.concatenate([near_values, values], axis=0)

    def pair_turn(turn_index, loop_carry):
        moving_keys, moving_values, inner_state = loop_carry
        moving_keys, moving_values = passed_along((moving_keys, moving_values), "seq", 2)
        key_first = own_first - (2 * turn_index + 3) * row_count
        inner_state = take_block(inner_state, moving_keys, moving_values, key_first)
        return (moving_keys, moving_values, inner_state)

    finished = lax.fori_loop(0, reach_blocks // 2, pair_turn, (pair_keys, pair_values, carry_state))
    carry_state = finished[2]
    row_max, row_sum, accum = carry_state
    attended = (accum / row_sum[..., None]).transpose(2, 0, 1, 3)
    attended = attended.reshape(row_count, queries.shape[1]).astype(jnp.bfloat16)
    mixed = jnp.dot(
        lax.all_gather(attended, "head", axis=1, tiled=True),
        out_weight,
        preferred_element_type=jnp.float32,
    )
    return mixed.astype(jnp.bfloat16)


SUBTILE = 16
REACH = 3
PAIRS = 4
VMEM_GRANT = 32 * 2**20


def needed_reach(token_count, row_count, cycle_size):
    back = token_count // 3 - 1
    return min(WIN_BLK, cycle_size - 1, -(-back // row_count))


def fused_kernel(
    reach, far_rows, cycle_size, q_hbm, k_hbm, v_hbm, seg_hbm, w_hbm, out_ref,
    q_ref, kv_ref, seg_ref, w_ref, att_ref, acc_ref,
    load_sem, w_sem, kv_send, kv_recv, att_send, att_recv,
):
    rows = k_hbm.shape[0]
    width = q_hbm.shape[1]
    group = width // HD
    pair_width = width // PAIRS
    seq = lax.axis_index("seq")
    head = lax.axis_index("head")
    x_at, y_at = head % 2, head // 2
    peers = (head, head + 1 - 2 * x_at, head + 2 - 4 * y_at, 3 - head)
    own_at = reach * rows

    core = seq % 2
    partner = seq + 1 - 2 * core
    has_next, has_last = seq + 2 < cycle_size, seq - 2 >= 0
    sends_far = (core == 1) & (seq + 3 < cycle_size)
    takes_far = (core == 0) & (seq - 3 >= 0)

    barrier = pltpu.get_barrier_semaphore()

    def greet(axis, place):
        pl.semaphore_signal(barrier, inc=1, device_id={axis: place})

    pl.when(has_next)(lambda: greet("seq", seq + 2))
    pl.when(has_last)(lambda: greet("seq", seq - 2))
    pl.when(sends_far)(lambda: greet("seq", seq + 3))
    pl.when(takes_far)(lambda: greet("seq", seq - 3))
    greet("head", peers[1])
    greet("head", peers[2])
    greet("seq", partner)

    own = [
        pltpu.make_async_copy(src, kv_ref.at[i, pl.ds(own_at, rows), :], load_sem.at[i])
        for i, src in enumerate((k_hbm, v_hbm))
    ]
    q_load = pltpu.make_async_copy(q_hbm, q_ref, load_sem.at[2])
    seg_load = pltpu.make_async_copy(seg_hbm, seg_ref, load_sem.at[3])
    for copy in own + [q_load, seg_load]:
        copy.start()
    w_loads = []
    for r, peer in enumerate(peers):
        first = pl.multiple_of(peer * width, width)
        w_loads.append(pltpu.make_async_copy(w_hbm.at[pl.ds(first, width), :], w_ref.at[r], w_sem.at[r]))
        w_loads[r].start()

    def kv_copy(held, d, i, target):
        skip = rows - far_rows if d == reach else 0
        return pltpu.make_async_remote_copy(
            src_ref=kv_ref.at[i, pl.ds(own_at - held * rows + skip, rows - skip), :],
            dst_ref=kv_ref.at[i, pl.ds(own_at - d * rows + skip, rows - skip), :],
            send_sem=kv_send.at[d - 1, i],
            recv_sem=kv_recv.at[d - 1, i],
            device_id={"seq": target},
        )

    if far_rows < rows:
        kv_ref[:, : rows - far_rows, :] = jnp.zeros((2, rows - far_rows, HD), jnp.bfloat16)
    for d in range(1, reach + 1):
        skip = rows - far_rows if d == reach else 0

        @pl.when(seq - d < 0)
        def _():
            kv_ref[:, pl.ds(own_at - d * rows + skip, rows - skip), :] = jnp.zeros(
                (2, rows - skip, HD), jnp.bfloat16)

    far_peer = core * jnp.minimum(1, (cycle_size - 1 - seq) // 3) + (1 - core) * jnp.minimum(1, seq // 3)
    near_peers = jnp.minimum(1, (cycle_size - 1 - seq) // 2) + jnp.minimum(1, seq // 2)
    pl.semaphore_wait(barrier, 3 + near_peers + far_peer)

    for i in range(2):
        own[i].wait()
        pl.when(has_next)(lambda i=i: kv_copy(0, 2, i, seq + 2).start())
        pl.when(sends_far)(lambda i=i: kv_copy(0, 3, i, seq + 3).start())
        pl.when(core == 0)(lambda i=i: kv_copy(0, 1, i, partner).start())

    seg_load.wait()
    length = (reach + 1) * rows
    key_seg = jnp.concatenate(
        [seg_ref[pl.ds((seq - d + cycle_size) % cycle_size, 1), :] for d in range(reach, -1, -1)], axis=1)
    seg_own = seg_ref[pl.ds(seq, 1), :]
    query_seg = jnp.broadcast_to(seg_own, (rows, rows)).T
    query_seg = jnp.concatenate([query_seg] * (reach + 1), axis=1)
    query_pos = seq * rows + lax.broadcasted_iota(jnp.int32, (rows, length), 0)
    key_pos = (seq - reach) * rows + lax.broadcasted_iota(jnp.int32, (rows, length), 1)
    allowed = (key_pos <= query_pos) & (query_pos - key_pos < WIN_BLK * rows) & (key_pos >= 0)
    allowed = allowed & (key_seg == query_seg)

    q_load.wait()

    def relay(i):
        @pl.when(has_last)
        def _():
            kv_copy(0, 2, i, partner).wait_recv()

            @pl.when(core == 0)
            def _():
                kv_copy(2, 3, i, partner).start()

            @pl.when(core == 1)
            def _():
                kv_copy(2, 1, i, partner).start()

    def arrivals(i):
        pl.when((core == 1) | has_last)(lambda: kv_copy(0, 1, i, partner).wait_recv())
        pl.when(((core == 1) & has_last) | takes_far)(lambda: kv_copy(0, 3, i, partner).wait_recv())

    relay(0)
    relay(1)
    arrivals(0)
    factor = HD ** (-0.5) * math.log2(math.e)

    def att_copy(held, r, c, target):
        return pltpu.make_async_remote_copy(
            src_ref=att_ref.at[held, c],
            dst_ref=att_ref.at[r, c],
            send_sem=att_send.at[r - 1, c],
            recv_sem=att_recv.at[r - 1, c],
            device_id={"head": peers[target]},
        )

    per_pair = group // PAIRS
    probs, totals = [], []
    for h in range(group):
        q_h = q_ref[:, h * HD:(h + 1) * HD]
        scores = lax.dot_general(
            q_h, kv_ref[0], (((1,), (1,)), ((), ())), preferred_element_type=jnp.float32)
        scores = jnp.where(allowed, scores, masked_score)
        row_max = jnp.max(scores, axis=1, keepdims=True)
        raw = jnp.exp2((scores - row_max) * factor)
        totals.append(jnp.sum(raw, axis=1, keepdims=True))
        probs.append(raw.astype(jnp.bfloat16))
    arrivals(1)
    half = PAIRS // 2
    first_out = {1: tuple(range(half)), 2: tuple(range(half, PAIRS))}
    turns = [(r, first_out[r][k]) for k in range(half) for r in (1, 2)]
    for r, c in turns:
        for place in range(per_pair):
            h = c * per_pair + place
            part = jnp.dot(probs[h], kv_ref[1], preferred_element_type=jnp.float32)
            att_ref[0, c, :, place * HD:(place + 1) * HD] = (part / totals[h]).astype(jnp.bfloat16)
        att_copy(0, r, c, r).start()
    for r, c in turns:
        att_copy(0, 3 - r, c, 3 - r).start()

    order = [(0, c) for c in range(PAIRS)] + turns + [(3 - r, c) for r, c in turns] + [(3, c) for _, c in turns]
    loaded = set()
    for step, (r, c) in enumerate(order):
        if r:
            att_copy(0, r, c, 1).wait_recv()
        if (r, c) in turns:
            att_copy(r, 3, c, 3 - r).start()
        if r not in loaded:
            w_loads[r].wait()
            loaded.add(r)
        piece = jnp.dot(
            att_ref[r, c], w_ref[r, c * pair_width:(c + 1) * pair_width, :],
            preferred_element_type=jnp.float32)
        if step == 0:
            acc_ref[...] = piece
        elif step < len(order) - 1:
            acc_ref[...] += piece
        else:
            out_ref[...] = (acc_ref[...] + piece).astype(jnp.bfloat16)

    for i in range(2):
        pl.when(has_next)(lambda i=i: kv_copy(0, 2, i, seq + 2).wait_send())
        pl.when(sends_far | ((core == 0) & has_last))(lambda i=i: kv_copy(0, 3, i, partner).wait_send())
        pl.when((core == 0) | has_last)(lambda i=i: kv_copy(0, 1, i, partner).wait_send())
    for r in range(1, 4):
        for c in range(PAIRS):
            att_copy(0, r, c, 1).wait_send()


def fused(reach, queries, keys, values, segments, out_weight):
    rows, width = queries.shape
    cycle_size = lax.axis_size("seq")
    features = out_weight.shape[1]
    back = segments.shape[0] // 3 - 1 - (reach - 1) * rows
    far_rows = min(rows, -(-back // SUBTILE) * SUBTILE)
    hbm_spec = pl.BlockSpec(memory_space=pltpu.HBM)
    pair_width = width // PAIRS
    operands = (queries, keys, values, segments.reshape(cycle_size, rows), out_weight)
    return pl.pallas_call(
        functools.partial(fused_kernel, reach, far_rows, cycle_size),
        out_shape=pltpu.VMEM((rows, features), jnp.bfloat16),
        in_specs=[hbm_spec] * 5,
        out_specs=pl.BlockSpec(memory_space=pltpu.VMEM),
        scratch_shapes=[
            pltpu.VMEM((rows, width), jnp.bfloat16),
            pltpu.VMEM((2, (reach + 1) * rows, HD), jnp.bfloat16),
            pltpu.VMEM((cycle_size, rows), jnp.int32),
            pltpu.VMEM((4, width, features), jnp.bfloat16),
            pltpu.VMEM((4, PAIRS, rows, pair_width), jnp.bfloat16),
            pltpu.VMEM((rows, features), jnp.float32),
            pltpu.SemaphoreType.DMA((4,)),
            pltpu.SemaphoreType.DMA((4,)),
            pltpu.SemaphoreType.DMA((reach, 2)),
            pltpu.SemaphoreType.DMA((reach, 2)),
            pltpu.SemaphoreType.DMA((3, PAIRS)),
            pltpu.SemaphoreType.DMA((3, PAIRS)),
        ],
        compiler_params=pltpu.CompilerParams(
            collective_id=0, has_side_effects=True, vmem_limit_bytes=VMEM_GRANT),
    )(*(pltpu.with_memory_space_constraint(a, pltpu.HBM) for a in operands))


def chosen(queries, keys, values, segments, out_weight):
    row_count, width = queries.shape
    cycle_size = lax.axis_size("seq")
    reach = needed_reach(segments.shape[0], row_count, cycle_size)
    fits = reach == REACH and cycle_size % 2 == 0 and lax.axis_size("head") == 4
    fits = fits and keys.shape[1] == HD and width % (PAIRS * HD) == 0
    if fits and row_count == HD and 4 * width == out_weight.shape[0]:
        return fused(reach, queries, keys, values, segments, out_weight)
    return on_device(queries, keys, values, segments, out_weight)


def solution(mesh):
    return jax.shard_map(
        chosen,
        mesh=mesh,
        in_specs=(P("seq", "head"), P("seq", "head"), P("seq", "head"), P(), P(None, "head")),
        out_specs=P("seq", "head"),
        check_vma=False,
    )
```
